256 devices in a mesh: dp: 16 (over z, core), seq: 4 (over x), section: 4 (over y).
Axes of the slice: x: 4, y: 4, z: 8, core: 2. Of those that a mesh axis runs over, the one named last changes fastest.
Arguments:
- projected: bfloat16 [4, 4, 96, 128, 4096], P('section', 'seq', 'dp'), may hold values from -6 to 6
- dest_owner: int32 [4, 4, 96], P('section', 'seq', 'dp'), may hold values from 0 to 15, as said below
- slot_from: int32 [4, 16, 24], P('section', 'dp', 'seq'), may hold values from 0 to 15, as said below
- doc_starts: int32 [4, 16, 24], P('section', 'dp', 'seq'), may hold values from 0 to 1, as said below
- live_rows: int32 [4, 16, 24], P('section', 'dp', 'seq'), may hold values from 1 to 128, as said below
Outputs:
- attended: bfloat16 [4, 16, 3072, 2048], P('section', 'dp', 'seq')
The draws below stay inside these ranges and needn't reach their ends.
Inputs may be any that keep to these rules, and one draw needn't show every extreme that they name: `dest_owner`: in each column (t, s), every source device sends at most 1 block to one owner, some source sends exactly 1 block to some owner, and every owner receives exactly 6 blocks. Over all 4 columns (t, s) of one section t, source a sends at most 2 blocks to one owner, and some source sends exactly 2 to some owner. For owner o in column (t, s), slot_from[t, o, s * 6 + j] over j names each of the 6 numbers of the blocks that went to o in that column once. `doc_starts`: the first block of every pack begins a document; a document spans at most 8 blocks, and in every pack some document spans exactly 8. `live_rows`: 128 in every block but the last block of a document (the block before the next start, or the pack's last block).
All inputs are finite; a program needn't handle non-finite values.
Results may differ from the reference program's by a relative error of at most 0.0069.
Values may be sent and summed in bfloat16 or wider, within the bound.
No kernel may reach another device: no remote copies, remote signals or barrier semaphores. Data moves between devices by JAX's collectives and lax.ppermute only.
A program may use at most 128 MiB of HBM per device.

```python
import jax
import jax.numpy as jnp
from jax import lax

HEADS = 8
KV_HEADS = 4
HEAD_DIM = 256
BLOCK = 128
DOC_MOST = 8
SRC_BLK = 6
SECTIONS = 4
SHARDS = 4
OWNERS = 16
SOURCES = 96
CAP = 1
PACK_BLK = 24
PACK_ROWS = 3072
WIDTH = 4096


def route_tables(key):
    section_keys = jax.random.split(jax.random.fold_in(key, 11), SECTIONS)

    def section_tables(section_key):
        subkeys = jax.random.split(section_key, 5)
        source_shift = jax.random.permutation(subkeys[0], OWNERS)
        owner_perm = jax.random.permutation(subkeys[1], OWNERS)
        offset_perm = jax.random.permutation(subkeys[2], OWNERS)
        shuffle_keys = jax.random.split(subkeys[3], SHARDS)
        order_keys = jax.random.split(subkeys[4], SHARDS)

        def column(shard_index, shuffle_key, order_key):
            offsets = offset_perm[(shard_index * SRC_BLK + jnp.arange(SRC_BLK, dtype=jnp.int32)) % OWNERS]

            def shuffle(subkey):
                return jax.random.permutation(subkey, SRC_BLK)
            shuffles = jax.vmap(shuffle)(jax.random.split(shuffle_key, OWNERS))
            owner_of = owner_perm[(source_shift[:, None] + offsets[shuffles]) % OWNERS].astype(jnp.int32)
            same_owner = owner_of[:, :, None] == owner_of[:, None, :]
            earlier = jnp.arange(SRC_BLK)[None, :] < jnp.arange(SRC_BLK)[:, None]
            ranking = jnp.sum(same_owner & earlier[None], axis=2).astype(jnp.int32)
            numbering = jnp.arange(OWNERS, dtype=jnp.int32)[:, None] * CAP + ranking
            flat_owner = owner_of.reshape(-1)
            tiebreak = jax.random.permutation(order_key, OWNERS * SRC_BLK).astype(jnp.int32)
            ordering = jnp.argsort(flat_owner * (OWNERS * SRC_BLK) + tiebreak, stable=True)
            slot_list = numbering.reshape(-1)[ordering].reshape(OWNERS, SRC_BLK)
            return (flat_owner, slot_list)
        return jax.vmap(column)(jnp.arange(SHARDS, dtype=jnp.int32), shuffle_keys, order_keys)
    owner_lists, slot_lists = jax.vmap(section_tables)(section_keys)
    owner_lists = owner_lists.reshape(SECTIONS, SHARDS, OWNERS * SRC_BLK)
    slot_lists = slot_lists.reshape(SECTIONS, SHARDS, OWNERS, SRC_BLK).transpose(0, 2, 1, 3).reshape(SECTIONS, OWNERS, PACK_BLK)
    return (owner_lists.astype(jnp.int32), slot_lists.astype(jnp.int32))


def document_tables(key):
    subkeys = jax.random.split(jax.random.fold_in(key, 23), 3)
    pack_count = SECTIONS * OWNERS
    lengths = jax.random.randint(subkeys[0], (pack_count, PACK_BLK), 1, DOC_MOST + 1)
    longest = jax.random.randint(subkeys[1], (pack_count, 1), 0, PACK_BLK // DOC_MOST)
    lengths = jnp.where(jnp.arange(PACK_BLK)[None, :] == longest, DOC_MOST, lengths)
    doc_ends = jnp.cumsum(lengths, axis=1)
    doc_begins = doc_ends - lengths
    block_ids = jnp.arange(PACK_BLK)
    start_flags = jnp.any(doc_begins[:, None, :] == block_ids[None, :, None], axis=2).astype(jnp.int32)
    closing = jnp.any(doc_ends[:, None, :] == (block_ids + 1)[None, :, None], axis=2) | (block_ids == PACK_BLK - 1)[None, :]
    tail_rows = jax.random.randint(subkeys[2], (pack_count, PACK_BLK), 1, BLOCK + 1)
    live_count = jnp.where(closing, tail_rows, BLOCK).astype(jnp.int32)
    return (start_flags.reshape(SECTIONS, OWNERS, PACK_BLK), live_count.reshape(SECTIONS, OWNERS, PACK_BLK))


def draw_projected(key, part):
    base_key = jax.random.fold_in(key, 37)
    half_width = HEAD_DIM // 2
    pair_index = jnp.arange(HEAD_DIM) % half_width
    slow_mask = (pair_index >= 3 * half_width // 4).astype(jnp.float32)
    direction = jnp.where(jax.random.bernoulli(jax.random.fold_in(key, 41), 0.5, (KV_HEADS, HEAD_DIM)), 1.0, -1.0)
    pattern = direction * slow_mask[None, :]
    group_size = HEADS // KV_HEADS

    def slab(number):
        slab_keys = jax.random.split(jax.random.fold_in(base_key, number), 4)
        noise_part = jax.random.normal(slab_keys[0], (SOURCES, BLOCK, WIDTH), jnp.float32)
        strength = jax.random.uniform(slab_keys[1], (SOURCES, BLOCK, 1), jnp.float32, 2.0, 3.5)
        picked = jax.random.bernoulli(slab_keys[2], 0.125, (SOURCES, BLOCK, 1))
        sign_flip = jnp.where(jax.random.bernoulli(slab_keys[3], 0.5, (SOURCES, BLOCK, KV_HEADS)), 1.0, -1.0)
        amount = jnp.where(picked, strength, 0.0) * sign_flip
        shared = amount[:, :, :, None] * pattern[None, None, :, :]
        query_add = jnp.broadcast_to(shared[:, :, :, None, :], (SOURCES, BLOCK, KV_HEADS, group_size, HEAD_DIM)).reshape(SOURCES, BLOCK, HEADS * HEAD_DIM)
        key_add = shared.reshape(SOURCES, BLOCK, KV_HEADS * HEAD_DIM)
        value_add = jnp.zeros((SOURCES, BLOCK, KV_HEADS * HEAD_DIM), jnp.float32)
        combined = noise_part + jnp.concatenate([query_add, key_add, value_add], axis=2)
        return jnp.clip(combined, -6.0, 6.0).astype(jnp.bfloat16)
    slabs = lax.map(slab, jnp.arange(SECTIONS * SHARDS, dtype=jnp.int32))
    return slabs.reshape(SECTIONS, SHARDS, SOURCES, BLOCK, WIDTH)


def draw_dest_owner(key, part):
    return route_tables(key)[0]


def draw_slot_from(key, part):
    return route_tables(key)[1]


def draw_doc_starts(key, part):
    return document_tables(key)[0]


def draw_live_rows(key, part):
    return document_tables(key)[1]


def setup_inputs(seed: int = 0) -> dict:
    keys = jax.random.split(jax.random.key(seed), 6)
    projected = draw_projected(jax.random.fold_in(keys[5], 71), 0)
    dest_owner = draw_dest_owner(jax.random.fold_in(keys[5], 71), 0)
    slot_from = draw_slot_from(jax.random.fold_in(keys[5], 71), 0)
    doc_starts = draw_doc_starts(jax.random.fold_in(keys[5], 71), 0)
    live_rows = draw_live_rows(jax.random.fold_in(keys[5], 71), 0)
    return dict(projected=projected, dest_owner=dest_owner, slot_from=slot_from, doc_starts=doc_starts, live_rows=live_rows)


score_cap = 50.0
rope_base = 10000.0


def rotate(columns, position, head_count):
    row_count = columns.shape[0]
    head_width = columns.shape[1] // head_count
    half_width = head_width // 2
    frequency = rope_base ** (-2.0 * jnp.arange(half_width, dtype=jnp.float32) / head_width)
    angles = position[:, None] * frequency[None, :]
    cosine = jnp.cos(angles)[:, None, :]
    sine_part = jnp.sin(angles)[:, None, :]
    split_heads = columns.astype(jnp.float32).reshape(row_count, head_count, head_width)
    first_half = split_heads[:, :, :half_width]
    second_half = split_heads[:, :, half_width:]
    turned = jnp.concatenate([first_half * cosine - second_half * sine_part, second_half * cosine + first_half * sine_part], axis=2)
    return turned.reshape(row_count, head_count * head_width).astype(jnp.bfloat16)


def source_choice(owner_list, slot_list):
    owner_grid = owner_list.reshape(OWNERS, SRC_BLK)
    same_owner = owner_grid[:, :, None] == owner_grid[:, None, :]
    earlier = jnp.arange(SRC_BLK)[None, :] < jnp.arange(SRC_BLK)[:, None]
    ranking = jnp.sum(same_owner & earlier[None], axis=2).astype(jnp.int32)
    located = owner_grid * (OWNERS * CAP) + jnp.arange(OWNERS, dtype=jnp.int32)[:, None] * CAP + ranking
    lookup = jnp.zeros((OWNERS * OWNERS * CAP,), jnp.int32).at[located.reshape(-1)].set(jnp.arange(OWNERS * SRC_BLK, dtype=jnp.int32))
    return lookup[jnp.arange(OWNERS, dtype=jnp.int32)[:, None] * (OWNERS * CAP) + slot_list]


def attend_pack(pack_rows, start_flags, live_count):
    query_width = HEADS * HEAD_DIM
    key_width = KV_HEADS * HEAD_DIM
    group_size = HEADS // KV_HEADS
    block_ids = jnp.arange(PACK_BLK, dtype=jnp.int32)
    doc_number = jnp.cumsum(start_flags).astype(jnp.int32) - 1
    doc_first = lax.cummax(jnp.where(start_flags == 1, block_ids, -1), axis=0)
    row_offset = jnp.arange(BLOCK, dtype=jnp.int32)
    position = ((block_ids - doc_first)[:, None] * BLOCK + row_offset[None, :]).reshape(-1).astype(jnp.float32)
    alive_rows = (row_offset[None, :] < live_count[:, None]).reshape(-1)
    doc_rows = jnp.repeat(doc_number, BLOCK)
    query_tag = jnp.where(alive_rows, doc_rows, -2)
    key_tag = jnp.where(alive_rows, doc_rows, -1)
    queries = rotate(pack_rows[:, :query_width], position, HEADS)
    key_rows = rotate(pack_rows[:, query_width:query_width + key_width], position, KV_HEADS)
    values = pack_rows[:, query_width + key_width:]
    margin = (DOC_MOST - 1) * BLOCK
    key_rows = jnp.concatenate([jnp.zeros((margin, key_width), key_rows.dtype), key_rows])
    values = jnp.concatenate([jnp.zeros((margin, key_width), values.dtype), values])
    key_tag = jnp.concatenate([jnp.full((margin,), -1, jnp.int32), key_tag])
    key_index = jnp.arange(PACK_ROWS + margin, dtype=jnp.int32) - margin
    query_index = jnp.arange(PACK_ROWS, dtype=jnp.int32)
    window = DOC_MOST * BLOCK

    def one_block(number):
        begin_row = number * BLOCK
        query_part = lax.dynamic_slice_in_dim(queries, begin_row, BLOCK, 0)
        key_part = lax.dynamic_slice_in_dim(key_rows, begin_row, window, 0)
        value_part = lax.dynamic_slice_in_dim(values, begin_row, window, 0)
        query_tags = lax.dynamic_slice_in_dim(query_tag, begin_row, BLOCK, 0)
        key_tags = lax.dynamic_slice_in_dim(key_tag, begin_row, window, 0)
        query_rows = lax.dynamic_slice_in_dim(query_index, begin_row, BLOCK, 0)
        key_rows_here = lax.dynamic_slice_in_dim(key_index, begin_row, window, 0)
        alive_here = lax.dynamic_slice_in_dim(alive_rows, begin_row, BLOCK, 0)
        grouped = lax.optimization_barrier(query_part).astype(jnp.float32).reshape(BLOCK, KV_HEADS, group_size, HEAD_DIM)
        keyed = lax.optimization_barrier(key_part).astype(jnp.float32).reshape(window, KV_HEADS, HEAD_DIM)
        scores = jnp.einsum("rhgd,khd->rhgk", grouped, keyed, precision=lax.Precision.HIGHEST) * HEAD_DIM ** -0.5
        capped = score_cap * jnp.tanh(scores / score_cap)
        allowed = (query_tags[:, None] == key_tags[None, :]) & (key_rows_here[None, :] <= query_rows[:, None])
        weight = jnp.where(allowed[:, None, None, :], jnp.exp(capped), 0.0)
        denominator = jnp.sum(weight, axis=3)
        rounded = lax.optimization_barrier(weight.astype(jnp.bfloat16)).astype(jnp.float32)
        valued = value_part.astype(jnp.float32).reshape(window, KV_HEADS, HEAD_DIM)
        numerator = jnp.einsum("rhgk,khd->rhgd", rounded, valued, precision=lax.Precision.HIGHEST)
        safe_total = jnp.where(alive_here[:, None, None], denominator, 1.0)
        averaged = jnp.where(alive_here[:, None, None, None], numerator / safe_total[:, :, :, None], 0.0)
        return averaged.reshape(BLOCK, query_width).astype(jnp.bfloat16)

    return lax.map(one_block, block_ids).reshape(PACK_ROWS, query_width)


def reference(projected, dest_owner, slot_from, doc_starts, live_rows):
    column_slots = slot_from.reshape(SECTIONS, OWNERS, SHARDS, SRC_BLK).transpose(0, 2, 1, 3)
    chosen = jax.vmap(jax.vmap(source_choice))(dest_owner, column_slots)

    def one_pack(number):
        section_index = number // OWNERS
        owner_index = number % OWNERS
        picks = chosen[section_index][:, owner_index]
        gathered = projected[section_index][jnp.arange(SHARDS, dtype=jnp.int32)[:, None], picks]
        pack_rows = gathered.reshape(PACK_ROWS, WIDTH)
        return attend_pack(pack_rows, doc_starts[section_index, owner_index], live_rows[section_index, owner_index])

    results = lax.map(one_pack, jnp.arange(SECTIONS * OWNERS, dtype=jnp.int32))
    results = results.reshape(SECTIONS, OWNERS, PACK_ROWS, HEADS * HEAD_DIM)
    return jnp.roll(results, 1, axis=0)
```

```python
import jax
import jax.numpy as jnp
from jax import lax
from jax.experimental import pallas as pl
from jax.experimental.pallas import tpu as pltpu
from jax.sharding import PartitionSpec as P


HEADS = 8
KV_HEADS = 4
HEAD_DIM = 256
BLOCK = 128
DOC_MOST = 8

SCORE_CAP = 50.0
ROPE_BASE = 10000.0
LOG2_E = 1.4426950408889634


VMEM = pltpu.VMEM
SMEM = pltpu.SMEM


def whole(space):
    return pl.BlockSpec(memory_space=space)


def seq_shift(array, distance):
    n = lax.axis_size("seq")
    return lax.ppermute(array, "seq", [(i, (i + distance) % n) for i in range(n)])


def section_shift(array):
    n = lax.axis_size("section")
    return lax.ppermute(array, "section", [(i, (i + 1) % n) for i in range(n)])


def both_shift(array, distance):
    m, n = lax.axis_size("section"), lax.axis_size("seq")
    route = [
        (s * m + t, ((s + distance) % n) * m + (t + 1) % m) for s in range(n) for t in range(m)
    ]
    return lax.ppermute(array, ("seq", "section"), route)


def cost(flops, bytes_accessed, transcendentals=0):
    return pl.CostEstimate(
        flops=int(flops), bytes_accessed=int(bytes_accessed), transcendentals=int(transcendentals)
    )


def outgoing(chosen, groups):
    slots = chosen.shape[0]
    rows, width = groups[0][0].shape
    blocks = rows // BLOCK
    pieces = len(groups[0])
    total = width * len(groups)

    def kernel(chosen_ref, *refs):
        out_ref = refs[-1]

        def slot(i, carry):
            pick = chosen_ref[i]
            piece = pick // blocks
            start = pl.multiple_of((pick % blocks) * BLOCK, BLOCK)
            for d in range(pieces):

                @pl.when(piece == d)
                def _():
                    for g in range(len(groups)):
                        out_ref[i, :, g * width : (g + 1) * width] = refs[g * pieces + d][
                            pl.ds(start, BLOCK), :
                        ]

            return carry

        lax.fori_loop(0, slots, slot, 0)

    flat = [piece for group in groups for piece in group]
    moved = 2 * BLOCK * total * (slots + blocks * pieces)
    return pl.pallas_call(
        kernel,
        out_shape=jax.ShapeDtypeStruct((slots, BLOCK, total), flat[0].dtype),
        in_specs=[whole(SMEM)] + [whole(VMEM)] * len(flat),
        out_specs=whole(VMEM),
        cost_estimate=cost(3e6, moved),
    )(chosen, *flat)


def turned(block, cosine, sine):
    half = HEAD_DIM // 2
    first = block[:, :half].astype(jnp.float32)
    second = block[:, half:].astype(jnp.float32)
    return jnp.concatenate(
        [first * cosine - second * sine, second * cosine + first * sine], axis=1
    ).astype(jnp.bfloat16)


def pack_keys(slot_rows, offset, arrived, cosine, sine):
    count = slot_rows.shape[0]

    def kernel(slot_ref, offset_ref, arrived_ref, cos_ref, sin_ref, out_ref):
        def block(p, carry):
            at = pl.multiple_of(offset_ref[p] * BLOCK, BLOCK)
            to = pl.multiple_of(p * BLOCK, BLOCK)
            out_ref[pl.ds(to, BLOCK), :] = turned(
                arrived_ref[slot_ref[p]], cos_ref[pl.ds(at, BLOCK), :], sin_ref[pl.ds(at, BLOCK), :]
            )
            return carry

        lax.fori_loop(0, count, block, 0)

    return pl.pallas_call(
        kernel,
        out_shape=jax.ShapeDtypeStruct((count * BLOCK, HEAD_DIM), arrived.dtype),
        in_specs=[whole(SMEM)] * 2 + [whole(VMEM)] * 3,
        out_specs=whole(VMEM),
        cost_estimate=cost(1e7, 5e6),
        name="pack_keys",
    )(slot_rows, offset, arrived, cosine, sine)


def attend(tables, shard, queries, query_column, keys, arrived, cosine, sine, blocks):
    count = keys.shape[0] // BLOCK
    window = DOC_MOST - 1 + blocks
    most_pairs = DOC_MOST // 2
    arg_scale = HEAD_DIM**-0.5 / SCORE_CAP
    exp_scale = SCORE_CAP * LOG2_E

    def kernel(
        table_ref, shard_ref, q_ref, k_ref, v_ref, cos_ref, sin_ref, out_ref,
        q_buf, k_buf, v_buf, cos_buf, sin_buf, q_sems, v_sems, sems,
    ):
        begin = shard_ref[0] * blocks
        low = jnp.clip(begin - (DOC_MOST - 1), 0, count - window)
        copies = [
            pltpu.make_async_copy(
                k_ref.at[pl.ds(pl.multiple_of(low * BLOCK, BLOCK), window * BLOCK), :],
                k_buf,
                sems.at[0],
            ),
            pltpu.make_async_copy(cos_ref, cos_buf, sems.at[1]),
            pltpu.make_async_copy(sin_ref, sin_buf, sems.at[2]),
        ]
        for i in range(blocks):
            copies.append(
                pltpu.make_async_copy(
                    q_ref.at[table_ref[0, begin + i], :, pl.ds(query_column, HEAD_DIM)],
                    q_buf.at[i],
                    q_sems.at[i],
                )
            )
        for i in range(window):
            copies.append(
                pltpu.make_async_copy(
                    v_ref.at[table_ref[0, low + i], :, pl.ds(0, HEAD_DIM)],
                    v_buf.at[pl.ds(i * BLOCK, BLOCK), :],
                    v_sems.at[i],
                )
            )
        for copy in copies:
            copy.start()
        row = lax.broadcasted_iota(jnp.int32, (BLOCK, BLOCK), 0)
        col = lax.broadcasted_iota(jnp.int32, (BLOCK, BLOCK), 1)
        ahead = col - row
        row_of = lax.broadcasted_iota(jnp.int32, (BLOCK, HEAD_DIM), 0)
        for copy in copies:
            copy.wait()

        def block(i, carry):
            p = begin + i
            at = pl.multiple_of(table_ref[1, p] * BLOCK, BLOCK)
            first = table_ref[2, p]
            live = table_ref[3, p]
            query = turned(
                q_buf[i], cos_buf[pl.ds(at, BLOCK), :], sin_buf[pl.ds(at, BLOCK), :]
            )
            pairs = (p - first + 2) // 2
            to = pl.multiple_of(i * BLOCK, BLOCK)
            for n in range(1, most_pairs + 1):

                @pl.when(pairs == n)
                def _(n=n):
                    base = jnp.minimum(first, low + window - 2 * n)
                    start = pl.multiple_of((base - low) * BLOCK, BLOCK)
                    scores = lax.dot_general(
                        query,
                        k_buf[pl.ds(start, 2 * n * BLOCK), :],
                        (((1,), (1,)), ((), ())),
                        preferred_element_type=jnp.float32,
                    )
                    total = jnp.zeros((BLOCK, BLOCK), jnp.float32)
                    rounded = []
                    for k in range(2 * n):
                        key_block = base + k
                        limit = jnp.where(key_block >= first, table_ref[3, key_block], 0)
                        allowed = (col < limit) & (ahead <= (p - key_block) * BLOCK)
                        part = scores[:, k * BLOCK : (k + 1) * BLOCK]
                        weight = jnp.where(
                            allowed, jnp.exp2(jnp.tanh(part * arg_scale) * exp_scale), 0.0
                        )
                        total = total + weight
                        rounded.append(weight.astype(jnp.bfloat16))
                    numerator = lax.dot_general(
                        jnp.concatenate(rounded, axis=1),
                        v_buf[pl.ds(start, 2 * n * BLOCK), :],
                        (((1,), (0,)), ((), ())),
                        preferred_element_type=jnp.float32,
                    )
                    alive = row_of < live
                    summed = jnp.sum(total, axis=1, keepdims=True)
                    safe = jnp.where(alive[:, :1], summed, 1.0)
                    out_ref[pl.ds(to, BLOCK), :] = jnp.where(
                        alive, numerator / safe, 0.0
                    ).astype(jnp.bfloat16)

            return carry

        lax.fori_loop(0, blocks, block, 0)

    pairs = blocks * DOC_MOST / 2
    trig = (DOC_MOST * BLOCK, HEAD_DIM // 2)
    return pl.pallas_call(
        kernel,
        out_shape=jax.ShapeDtypeStruct((blocks * BLOCK, HEAD_DIM), keys.dtype),
        in_specs=[whole(SMEM)] * 2 + [whole(pl.ANY)] * 5,
        out_specs=whole(VMEM),
        scratch_shapes=[
            VMEM((blocks, BLOCK, HEAD_DIM), jnp.bfloat16),
            VMEM((window * BLOCK, HEAD_DIM), jnp.bfloat16),
            VMEM((window * BLOCK, HEAD_DIM), jnp.bfloat16),
            VMEM(trig, jnp.float32),
            VMEM(trig, jnp.float32),
            pltpu.SemaphoreType.DMA((blocks,)),
            pltpu.SemaphoreType.DMA((window,)),
            pltpu.SemaphoreType.DMA((3,)),
        ],
        cost_estimate=cost(
            pairs * 4 * BLOCK * BLOCK * HEAD_DIM, 4e6, pairs * 2 * BLOCK * BLOCK
        ),
        name="attend",
    )(tables, shard, queries, keys, arrived, cosine, sine)


def assemble(columns, pieces):
    rows, width = pieces[0].shape
    count = len(pieces)

    def kernel(column_ref, *refs):
        out_ref, sems = refs[count], refs[count + 1]
        copies = []
        for n in range(count):
            at = pl.multiple_of(column_ref[n] * width, width)
            copy = pltpu.make_async_copy(refs[n], out_ref.at[:, pl.ds(at, width)], sems.at[n])
            copy.start()
            copies.append(copy)
        for copy in copies:
            copy.wait()

    return pl.pallas_call(
        kernel,
        out_shape=jax.ShapeDtypeStruct((rows, width * count), pieces[0].dtype),
        in_specs=[whole(SMEM)] + [whole(VMEM)] * count,
        out_specs=whole(pl.ANY),
        scratch_shapes=[pltpu.SemaphoreType.DMA((count,))],
        cost_estimate=cost(1e6, 4 * rows * width * count),
        name="assemble",
    )(columns, *pieces)


def send_plan(owners, shard_count, blocks, me, pooled, dp_count):
    total = owners.shape[0]
    index = jnp.arange(total, dtype=jnp.int32)
    same = (owners[:, None] == owners[None, :]) & (index[None, :] < index[:, None])
    target = owners * pooled + jnp.sum(same, axis=1, dtype=jnp.int32)
    slots = jnp.arange(dp_count * pooled, dtype=jnp.int32)
    matches = target[None, :] == slots[:, None]
    distance = (me - index // blocks) % shard_count
    place = distance * blocks + index % blocks
    return jnp.sum(jnp.where(matches, place[None, :], 0), axis=1, dtype=jnp.int32)


def arrival_plan(slots, shard_of, capacity, pooled):
    source = slots // capacity
    before = jnp.sum(
        (shard_of[None, :] < shard_of[:, None]) & (source[None, :] == source[:, None]),
        axis=1,
        dtype=jnp.int32,
    )
    return source * pooled + before + slots % capacity


def shards(projected, dest_owner, slot_from, doc_starts, live_rows):
    source_blocks, block_rows, full_width = projected.shape[2:]
    rows = source_blocks * block_rows
    source = projected.reshape(rows, full_width)
    dp_count = lax.axis_size("dp")
    seq_count = lax.axis_size("seq")
    capacity = (source_blocks + dp_count - 1) // dp_count
    total_blocks = seq_count * source_blocks
    pooled = (total_blocks + dp_count - 1) // dp_count
    group = HEADS // KV_HEADS
    query_width = HEADS * HEAD_DIM
    key_width = KV_HEADS * HEAD_DIM
    me = lax.axis_index("seq")
    distances = range(seq_count)

    def part(base, stride, distance):
        at = base + ((me + distance) % seq_count) * stride
        return lax.dynamic_slice_in_dim(source, at, HEAD_DIM, 1)

    mine = jnp.stack([dest_owner[0, 0], slot_from[0, 0], doc_starts[0, 0], live_rows[0, 0]])
    before = section_shift(mine)
    pair = jnp.stack([mine, before])
    key_pieces, pairs, value_pieces = [], [], []
    query_pieces = [[] for _ in range(group)]
    for d in distances:
        piece = part(query_width, HEAD_DIM, d)
        key_pieces.append(seq_shift(piece, d) if d else piece)
        pairs.append(seq_shift(pair, d) if d else pair)
        value_pieces.append(both_shift(part(query_width + key_width, HEAD_DIM, d), d))
        for h in range(group):
            query_pieces[h].append(
                both_shift(part(h * HEAD_DIM, group * HEAD_DIM, d), d)
            )
    tables = jnp.stack(pairs)[(me - jnp.arange(seq_count, dtype=jnp.int32)) % seq_count]
    tables = tables.transpose(1, 2, 0, 3).reshape(2, 4, total_blocks)

    shard_of = jnp.repeat(jnp.arange(seq_count, dtype=jnp.int32), source_blocks)
    block_ids = jnp.arange(total_blocks, dtype=jnp.int32)

    def plans(tables):
        chosen = send_plan(tables[0], seq_count, source_blocks, me, pooled, dp_count)
        slot_rows = arrival_plan(tables[1], shard_of, capacity, pooled)
        first = lax.cummax(jnp.where(tables[2] == 1, block_ids, -1), axis=0)
        return chosen, jnp.stack([slot_rows, block_ids - first, first, tables[3]])

    chosen_here, plan_here = plans(tables[0])
    chosen_there, plan_there = plans(tables[1])

    def exchange(chosen, groups):
        sent = outgoing(chosen, groups)
        width = sent.shape[-1]
        sent = sent.reshape(dp_count, pooled, block_rows, width)
        got = lax.all_to_all(sent, "dp", split_axis=0, concat_axis=0, tiled=True)
        return got.reshape(dp_count * pooled, block_rows, width)

    frequency = ROPE_BASE ** (
        -2.0 * jnp.arange(HEAD_DIM // 2, dtype=jnp.float32) / HEAD_DIM
    )
    positions = jnp.arange(DOC_MOST * block_rows, dtype=jnp.float32)
    angles = positions[:, None] * frequency[None, :]
    cosine, sine = jnp.cos(angles), jnp.sin(angles)

    key_arrived = exchange(chosen_here, [key_pieces])
    value_arrived = exchange(chosen_there, [value_pieces, query_pieces[0]])
    query_arrived = exchange(chosen_there, [query_pieces[1]])
    keys = section_shift(pack_keys(plan_here[0], plan_here[1], key_arrived, cosine, sine))

    pieces, columns = [], []
    for h, (queries, column) in enumerate([(value_arrived, HEAD_DIM), (query_arrived, 0)]):
        for d in [2, 1, 3, 0]:
            shard = ((me + d) % seq_count).astype(jnp.int32).reshape(1)
            out = attend(
                plan_there, shard, queries, column, keys, value_arrived, cosine, sine,
                source_blocks,
            )
            pieces.append(out if d == 0 else seq_shift(out, d))
            columns.append(((me - d) % seq_count) * group + h)
    result = assemble(jnp.stack(columns).astype(jnp.int32), pieces)
    return result[None, None]


def solution(mesh):
    placed = (
        P("section", "seq", "dp", None, None),
        P("section", "seq", "dp"),
        P("section", "dp", "seq"),
        P("section", "dp", "seq"),
        P("section", "dp", "seq"),
    )

    return jax.shard_map(
        shards,
        mesh=mesh,
        in_specs=placed,
        out_specs=P("section", "dp", "seq", None),
        check_vma=False,
    )
```
